16 devices in a mesh: dp: 1, ep: 16 (over x, y, z, core).
Axes of the slice: x: 2, y: 2, z: 2, core: 2. Of those that a mesh axis runs over, the one named last changes fastest.
Arguments:
- x: bfloat16 [1, 16, 256, 4096], P('dp', 'ep')
- expert: int32 [1, 16, 256, 8], P('dp', 'ep')
- slot: int32 [1, 16, 256, 8], P('dp', 'ep')
- gate: float32 [1, 16, 256, 8], P('dp', 'ep')
- w_gate: bfloat16 [64, 4096, 1536], P('ep')
- w_up: bfloat16 [64, 4096, 1536], P('ep')
- w_down: bfloat16 [64, 1536, 4096], P('ep')
Outputs:
- y: bfloat16 [1, 16, 256, 4096], P('dp', 'ep')
All inputs are finite; a program needn't handle non-finite values.
Results may differ from the reference program's by a relative error of at most 0.009.
Values are sent between devices in bfloat16 or wider.
A program may use at most 2 GiB of HBM per device.

```python
import jax
import jax.numpy as jnp

MEMBERS = 16
TOKENS = 256
D = 4096
FF = 1536
TOP = 8
EXPERTS = 64
SLOTS = 5 * TOKENS * TOP // (4 * EXPERTS)


def setup_inputs(seed: int = 0, part: int = 0) -> dict:
    own, k1, k2, k3, k4, k5, k6 = jax.random.split(jax.random.key(seed), 7)
    kx, ke, kl, kg = jax.random.split(jax.random.fold_in(own, part), 4)
    devices = (1, MEMBERS)
    place = jax.random.permutation(kl, jnp.arange(EXPERTS, dtype=jnp.uint32))
    slow = ((EXPERTS + (9 * place) % EXPERTS) << ((9 * place) // EXPERTS)) // EXPERTS
    wait = (jax.random.bits(ke, (*devices, TOKENS, EXPERTS), jnp.uint32) >> 10) * slow
    expert = jnp.argsort(wait, axis=-1)[..., :TOP].astype(jnp.int32)
    chosen = jax.nn.one_hot(expert, EXPERTS, dtype=jnp.int32)
    in_line = jnp.cumsum(chosen.reshape(*devices, TOKENS * TOP, EXPERTS), axis=2) - 1
    slot = jnp.sum(in_line.reshape(chosen.shape) * chosen, axis=-1)

    def one(key, rows, columns):
        return (jax.random.normal(key, (rows, columns), jnp.float32) * rows**-0.5).astype(jnp.bfloat16)

    def weights(key, rows, columns):
        return jax.lax.map(lambda k: one(k, rows, columns), jax.random.split(key, EXPERTS))

    return {
        "x": jax.random.normal(kx, (*devices, TOKENS, D), jnp.float32).astype(jnp.bfloat16),
        "expert": expert,
        "slot": slot,
        "gate": jax.nn.softmax(jax.random.normal(kg, expert.shape, jnp.float32)),
        "w_gate": weights(k1, D, FF),
        "w_up": weights(k2, D, FF),
        "w_down": weights(k3, FF, D),
    }


def einsum(form, a, b):
    return jnp.einsum(form, a.astype(jnp.float32), b.astype(jnp.float32))


def reference(x, expert, slot, gate, w_gate, w_up, w_down):
    to_expert = jax.nn.one_hot(expert, EXPERTS, dtype=jnp.bfloat16)
    to_slot = jax.nn.one_hot(slot, SLOTS, dtype=jnp.bfloat16)
    weighted = to_expert * gate[..., None].astype(jnp.bfloat16)
    dispatch = einsum("abtke,abtkc->abtec", to_expert, to_slot).astype(jnp.bfloat16)
    combine = einsum("abtke,abtkc->abtec", weighted, to_slot).astype(jnp.bfloat16)
    z = einsum("abtec,abtd->aebcd", dispatch, x).astype(jnp.bfloat16)
    h = jax.nn.silu(einsum("aebcd,edf->aebcf", z, w_gate))
    h = (h * einsum("aebcd,edf->aebcf", z, w_up)).astype(jnp.bfloat16)
    out = einsum("aebcf,efd->aebcd", h, w_down).astype(jnp.bfloat16)
    y = einsum("abtec,aebcd->abtd", combine, out)
    return y.astype(jnp.bfloat16)
```

```python
import functools

import jax
import jax.numpy as jnp
import numpy as np
from jax import lax
from jax.experimental import pallas as pl
from jax.experimental.pallas import tpu as pltpu
from jax.sharding import PartitionSpec as P

MESH = pl.DeviceIdType.MESH
CHIPS = 8
WEIGHT = (8, 4, 2)
ROWS = ((0, 88), (88, 88), (176, 80))
KC = 512


def bit(me, d):
    return lax.rem(me // WEIGHT[d], 2)


def flip(me, d):
    return me + WEIGHT[d] * (1 - 2 * bit(me, d))


def gather_kernel(
    slots, x_ref, meta_ref, rid_ref, wg_ref, wu_ref,
    xg_ref, c_ref, h_ref,
    allm, dmat, cbuf, own, xb, z, wg, wu, acc_g, acc_u, hb,
    s1, s2, s3, d2d, send, meta_send, meta_recv, own_sem, c_sem, x_sem, w_sem, h_sem,
):
    me = lax.axis_index("ep")
    core = lax.rem(me, 2)
    chip = me // 2
    partner = me + 1 - 2 * core
    tokens, depth = x_ref.shape
    chunks = depth // KC
    experts, _, ff = wg_ref.shape
    pair = 2 * slots
    rows = experts * pair

    def cols(j):
        return pl.ds(pl.multiple_of(j * KC, KC), KC)

    def part(idx, r, j):
        return xg_ref.at[idx // 2, lax.rem(idx, 2), pl.ds(*ROWS[r]), cols(j)]

    def own_part(r, j):
        return x_ref.at[pl.ds(*ROWS[r]), cols(j)]

    def push(src, idx, r, j, sem, to):
        pltpu.make_async_remote_copy(
            src_ref=src, dst_ref=part(idx, r, j), send_sem=send, recv_sem=sem.at[j, r],
            device_id={"ep": to}, device_id_type=MESH,
        ).start()

    def await_parts(n, r, j, sem):
        ref = xg_ref.at[pl.ds(0, n), 0, pl.ds(*ROWS[r]), cols(j)]
        pltpu.make_async_copy(ref, ref, sem.at[j, r]).wait()

    def stage_a(j):
        for r in range(3):
            push(own_part(r, j), me, r, j, s1, flip(me, r))
        for r in range(3):
            push(own_part(r, j), me, r, j, s2, flip(me, (r + 1) % 3))
        for r in range(3):
            push(own_part(r, j), me, r, j, s3, flip(me, (r + 2) % 3))

    def stage_b(j):
        for r in range(3):
            await_parts(1, r, j, s1)
            a = flip(me, r)
            push(part(a, r, j), a, r, j, s2, flip(me, (r + 1) % 3))
            push(part(a, r, j), a, r, j, s3, flip(me, (r + 2) % 3))

    def stage_c(j):
        for r in range(3):
            await_parts(2, r, j, s2)
            b = flip(me, (r + 1) % 3)
            ab = flip(b, r)
            push(part(b, r, j), b, r, j, s3, flip(me, (r + 2) % 3))
            push(part(ab, r, j), ab, r, j, s3, flip(me, (r + 2) % 3))

    def stage_e(j):
        for r in range(3):
            await_parts(4, r, j, s3)
        ref = xg_ref.at[:, core, :, cols(j)]
        pltpu.make_async_remote_copy(
            src_ref=ref, dst_ref=ref, send_sem=send, recv_sem=d2d.at[j],
            device_id={"ep": partner}, device_id_type=MESH,
        ).start()

    def await_d2d(j):
        ref = xg_ref.at[:, 0, :, cols(j)]
        pltpu.make_async_copy(ref, ref, d2d.at[j]).wait()

    def load_x(j):
        k = lax.rem(j, 2)
        return pltpu.make_async_copy(xg_ref.at[:, :, :, cols(j)], xb.at[k], x_sem.at[k])

    def load_w(q):
        j, e, k = q // experts, lax.rem(q, experts), lax.rem(q, 2)
        src = pl.ds(pl.multiple_of(j * KC, KC), KC)
        return (
            pltpu.make_async_copy(wg_ref.at[e, src, :], wg.at[k], w_sem.at[0, k]),
            pltpu.make_async_copy(wu_ref.at[e, src, :], wu.at[k], w_sem.at[1, k]),
        )

    def own_copy(i):
        half = tokens // 2
        at = pl.ds(i * half, half)
        a = pltpu.make_async_copy(x_ref.at[at, :], own, own_sem)
        a.start()
        a.wait()
        b = pltpu.make_async_copy(own, xg_ref.at[chip, core, at, :], own_sem)
        b.start()
        b.wait()

    barrier = pltpu.get_barrier_semaphore()
    for d in range(1, 16):
        pl.semaphore_signal(barrier, inc=1, device_id={"ep": lax.rem(me + d, 16)}, device_id_type=MESH)
    pl.semaphore_wait(barrier, 15)

    stage_a(0)
    for d in range(1, 16):
        pltpu.make_async_remote_copy(
            src_ref=meta_ref, dst_ref=allm.at[me], send_sem=meta_send, recv_sem=meta_recv,
            device_id={"ep": lax.rem(me + d, 16)}, device_id_type=MESH,
        ).start()
    stage_a(1)
    for w in load_w(0):
        w.start()
    mine = pltpu.make_async_copy(meta_ref, allm.at[me], own_sem)
    mine.start()
    mine.wait()
    own_copy(0)
    own_copy(1)
    stage_b(0)

    acc_g[...] = jnp.zeros_like(acc_g)
    acc_u[...] = jnp.zeros_like(acc_u)
    others = allm.at[pl.ds(0, 15)]
    pltpu.make_async_copy(others, others, meta_recv).wait()
    pltpu.make_async_copy(others, others, meta_send).wait()
    stage_a(2)
    stage_b(1)
    stage_c(0)

    base = (me * (experts * slots)).astype(jnp.float32)
    for s2_ in range(2):
        rid = rid_ref[s2_]
        rid = jnp.concatenate([rid, rid], axis=1)
        rid = jnp.where(rid < 0, rid, rid + base)

        @pl.loop(0, CHIPS)
        def _(p):
            m = allm[2 * p + s2_]
            d = jnp.zeros((rows, tokens), jnp.float32)
            c = jnp.zeros((rows, tokens), jnp.float32)
            for k in range(8):
                hit = rid == m[k:k + 1, :]
                d = jnp.where(hit, 1.0, d)
                c = jnp.where(hit, m[8 + k:9 + k, :], c)
            dmat[p, :, s2_ * tokens:(s2_ + 1) * tokens] = d.astype(jnp.bfloat16)
            cbuf[p, s2_] = c.T.astype(jnp.bfloat16)

    put_c = pltpu.make_async_copy(cbuf, c_ref, c_sem)
    put_c.start()

    def step(i, _):
        live = i >= 1
        j = jnp.maximum(i - 1, 0)
        k = lax.rem(j, 2)

        @pl.when(live)
        def _():
            load_x(j).wait()

            @pl.loop(0, CHIPS)
            def _(p):
                tok = xb[k, p].reshape(2 * tokens, KC)
                got = jnp.dot(dmat[p], tok, preferred_element_type=jnp.float32).astype(jnp.bfloat16)
                at = pl.ds(pl.multiple_of(p * pair, 16), pair)
                for e in range(experts):
                    z[e, at, :] = got[e * pair:(e + 1) * pair]

        def expert(e):
            @pl.when(live)
            def _():
                q = j * experts + e
                kw = lax.rem(q, 2)
                for w in load_w(q):
                    w.wait()

                @pl.when(q + 1 < chunks * experts)
                def _():
                    for w in load_w(q + 1):
                        w.start()

                @pl.loop(0, ff // 512)
                def _(n):
                    at = pl.ds(pl.multiple_of(n * 512, 512), 512)
                    acc_g[e, :, at] += jnp.dot(z[e], wg[kw, :, at], preferred_element_type=jnp.float32)
                    acc_u[e, :, at] += jnp.dot(z[e], wu[kw, :, at], preferred_element_type=jnp.float32)

        expert(0)

        @pl.when(i + 3 < chunks)
        def _():
            stage_a(i + 3)

        @pl.when(i + 2 < chunks)
        def _():
            stage_b(i + 2)

        expert(1)

        @pl.when(i < chunks)
        def _():
            stage_e(i)

        expert(2)

        @pl.when(i + 1 < chunks)
        def _():
            stage_c(i + 1)

        expert(3)

        @pl.when(i < chunks)
        def _():
            await_d2d(i)
            load_x(i).start()

        return 0

    lax.fori_loop(0, chunks + 1, step, 0)

    for e in range(experts):
        put = pltpu.make_async_copy(hb.at[e % 2], h_ref.at[e], h_sem.at[e % 2])
        if e >= 2:
            put.wait()

        @pl.loop(0, 8)
        def _(b):
            at = pl.ds(pl.multiple_of(b * pair, 16), pair)
            g = acc_g[e, at, :]
            hb[e % 2, at, :] = (g / (1.0 + jnp.exp(-g)) * acc_u[e, at, :]).astype(jnp.bfloat16)

        put.start()
    put_c.wait()
    for e in range(experts - 2, experts):
        pltpu.make_async_copy(hb.at[e % 2], h_ref.at[e], h_sem.at[e % 2]).wait()
    sent = xg_ref.at[:, :, :, pl.ds(0, depth - depth // 16)]
    pltpu.make_async_copy(sent, sent, send).wait()


ANY = pl.BlockSpec(memory_space=pl.ANY)
VM = pl.BlockSpec(memory_space=pltpu.VMEM)


def gather_call(slots, x, meta, rid, wg, wu):
    tokens, depth = x.shape
    experts, _, ff = wg.shape
    chunks = depth // KC
    rows = experts * 2 * slots
    per = 16 * slots
    bf, f32 = jnp.bfloat16, jnp.float32
    dma = pltpu.SemaphoreType.DMA
    return pl.pallas_call(
        functools.partial(gather_kernel, slots),
        out_shape=(
            jax.ShapeDtypeStruct((CHIPS, 2, tokens, depth), bf),
            jax.ShapeDtypeStruct((CHIPS, 2, tokens, rows), bf),
            jax.ShapeDtypeStruct((experts, per, ff), bf),
        ),
        in_specs=[ANY, VM, VM, ANY, ANY],
        out_specs=(ANY, ANY, ANY),
        scratch_shapes=[
            pltpu.VMEM((16, 16, tokens), f32),
            pltpu.VMEM((CHIPS, rows, 2 * tokens), bf),
            pltpu.VMEM((CHIPS, 2, tokens, rows), bf),
            pltpu.VMEM((tokens // 2, depth), bf),
            pltpu.VMEM((2, CHIPS, 2, tokens, KC), bf),
            pltpu.VMEM((experts, per, KC), bf),
            pltpu.VMEM((2, KC, ff), bf),
            pltpu.VMEM((2, KC, ff), bf),
            pltpu.VMEM((experts, per, ff), f32),
            pltpu.VMEM((experts, per, ff), f32),
            pltpu.VMEM((2, per, ff), bf),
            dma((chunks, 3)), dma((chunks, 3)), dma((chunks, 3)), dma((chunks,)),
            dma, dma, dma, dma, dma, dma((2,)), dma((2, 2)), dma((2,)),
        ],
        compiler_params=pltpu.CompilerParams(
            collective_id=0, has_side_effects=True, vmem_limit_bytes=67_000_000
        ),
        name="gather_up",
    )(x, meta, rid, wg, wu)


def np_rid(experts, slots):
    e, s, c = np.meshgrid(np.arange(experts), np.arange(2), np.arange(slots), indexing="ij")
    rid = np.where(s.reshape(1, -1) == np.arange(2)[:, None], (e * slots + c).reshape(1, -1), -7)
    return jnp.broadcast_to(jnp.asarray(rid, jnp.float32)[:, :, None], (*rid.shape, 128))


def solution(mesh):
    def step(x, expert, slot, gate, w_gate, w_up, w_down):
        x, expert, slot, gate = x[0, 0], expert[0, 0], slot[0, 0], gate[0, 0]
        tokens, top = expert.shape
        total = 16 * w_gate.shape[0]
        slots = 5 * tokens * top // (4 * total)
        number = jnp.where(slot < slots, expert * slots + slot, -1).astype(jnp.float32)
        weight = gate.astype(jnp.bfloat16).astype(jnp.float32)
        meta = jnp.concatenate([number.T, weight.T], axis=0)
        rid = np_rid(w_gate.shape[0], slots)
        xg, c, h = gather_call(slots, x, meta, rid, w_gate, w_up)
        out = jnp.einsum("erf,efd->erd", h, w_down, preferred_element_type=jnp.float32).astype(jnp.bfloat16)
        out = out.reshape(4, CHIPS, 2 * slots, -1).transpose(1, 0, 2, 3).reshape(CHIPS, 8 * slots, -1)
        y = jnp.einsum("pctr,prd->pctd", c, out, preferred_element_type=jnp.float32).astype(jnp.bfloat16)
        y = lax.psum_scatter(y.reshape(16, tokens, -1), "ep", scatter_dimension=0, tiled=False)
        return y[None, None]

    own = P("dp", "ep", None, None)
    return jax.shard_map(
        step, mesh=mesh,
        in_specs=(own, own, own, own, P("ep", None, None), P("ep", None, None), P("ep", None, None)),
        out_specs=own, check_vma=False,
    )
```
